32 devices in a mesh: blk: 32 (over z, y, x, core).
Axes of the slice: x: 2, y: 2, z: 4, core: 2. Of those that a mesh axis runs over, the one named last changes fastest.
Arguments:
- panel_left: bfloat16 [64, 64, 2048], P('blk'), may hold values from -0.75 to 0.75
- panel_right: bfloat16 [64, 64, 2048], P('blk'), may hold values from -0.125 to 0.125
- ranks: int32 [64], P('blk'), may hold values from 1 to 64
- rhs: float32 [64, 64, 2048], P('blk'), may hold values from -6 to 6
- pivot_left: bfloat16 [2048, 64], P('blk'), may hold values from -0.75 to 0.75
- pivot_right: bfloat16 [2048, 64], P('blk'), may hold values from -6 to 6
- finished: float32 [2048, 64], P('blk'), may hold values from -6 to 6
- pivot_rhs: float32 [2048, 64], P('blk'), may hold values from -6 to 6
- diag_inverse: float32 [2048, 2048], P('blk'), as said below
Outputs:
- new_left: bfloat16 [64, 64, 2048], P('blk')
- new_rhs: float32 [64, 64, 2048], P('blk')
- next_solution: float32 [2048, 64], P('blk')
The draws below stay inside these ranges and needn't reach their ends.
Inputs may be any that keep to these rules, and one draw needn't show every extreme that they name: diag_inverse is lower triangular with diagonal entries between 1 and 2.
All inputs are finite; a program needn't handle non-finite values.
Results may differ from the reference program's by a relative error of at most 0.0049.
Values sent between devices are 32-bit elements; how exact they have to be, the bound alone decides.
No kernel may reach another device: no remote copies, remote signals or barrier semaphores. Data moves between devices by JAX's collectives and lax.ppermute only.
A program may use at most 64 MiB of HBM per device.

```python
import jax
import jax.numpy as jnp
from jax import lax

NB = 2048
KMAX = 64
NRHS = 64
TILES = 64


def draw_diag_inverse(key, part):
    first = jax.random.fold_in(key, 11)
    second = jax.random.fold_in(key, 12)
    lower = jax.random.normal(first, (NB, NB), jnp.float32) * NB ** (-0.5)
    lower = jnp.tril(lower, -1)
    diag_vals = jax.random.uniform(second, (NB,), jnp.float32, 1.0, 2.0)
    return lower + jnp.diag(diag_vals)


def plant(values, rng, smallest, high):
    index_at = [jax.random.randint(jax.random.fold_in(rng, axis), (), 0, length) for axis, length in enumerate(values.shape)]
    widest = values.shape.index(max(values.shape))
    neighbour = index_at[:widest] + [(index_at[widest] + 1) % values.shape[widest]] + index_at[widest + 1:]
    return values.at[tuple(index_at)].set(smallest).at[tuple(neighbour)].set(high)


def block_scale(rng, dims, shards, smallest, high):
    level, own = 1.0, jax.random.fold_in(rng, 6)
    for position, parts in shards:
        steps = jnp.exp(jax.random.uniform(jax.random.fold_in(own, position), (parts,), jnp.float32, smallest / len(shards), high / len(shards)))
        level = level * jnp.repeat(steps, dims[position] // parts).reshape([-1 if axis == position else 1 for axis in range(len(dims))])
    return level


def noise(rng, extent, scale, limit, split=(), kind=jnp.bfloat16):
    level = block_scale(rng, extent, split, -0.22, 0.18) if split else 1.0
    drawn = jax.random.normal(rng, extent, jnp.float32) * scale * level
    return jnp.minimum(jnp.maximum(drawn, -limit), limit).astype(kind)


def setup_inputs(seed: int = 0) -> dict:
    seeds = jax.random.split(jax.random.key(seed), 10)
    return {
        "panel_left": noise(seeds[0], (TILES, KMAX, NB), KMAX ** -0.5, 0.75, ((0, 32),)),
        "panel_right": noise(seeds[1], (TILES, KMAX, NB), NB ** -0.5, 0.125, ((0, 32),)),
        "ranks": plant(jax.random.randint(seeds[2], (TILES,), 1, KMAX + 1), jax.random.fold_in(seeds[2], 1), 1, KMAX).astype(jnp.int32),
        "rhs": noise(seeds[3], (TILES, NRHS, NB), 1.0, 6.0, ((0, 32),), jnp.float32),
        "pivot_left": noise(seeds[4], (NB, KMAX), KMAX ** -0.5, 0.75, ((0, 32),)),
        "pivot_right": noise(seeds[5], (NB, KMAX), 1.0, 6.0, ((0, 32),)),
        "finished": noise(seeds[6], (NB, NRHS), 1.0, 6.0, ((0, 32),), jnp.float32),
        "pivot_rhs": noise(seeds[7], (NB, NRHS), 1.0, 6.0, ((0, 32),), jnp.float32),
        "diag_inverse": draw_diag_inverse(jax.random.fold_in(seeds[9], 71), 0),
    }


HIGH = lax.Precision.HIGHEST


def reference(panel_left, panel_right, ranks, rhs, pivot_left, pivot_right, finished, pivot_rhs, diag_inverse):
    columns = jnp.arange(KMAX, dtype=jnp.int32)
    pivot_wide = pivot_right.astype(jnp.float32)

    def one_tile(items):
        left, right, rank, right_side = items
        mask = (columns < rank).astype(jnp.bfloat16)
        left_m = (left * mask[:, None]).astype(jnp.float32)
        right_m = (right * mask[:, None]).astype(jnp.float32)
        gram = jnp.dot(right_m, pivot_wide, precision=HIGH).astype(jnp.bfloat16)
        proj = jnp.dot(right_m, finished, precision=HIGH)
        newl = jnp.dot(gram.astype(jnp.float32).T, left_m, precision=HIGH).astype(jnp.bfloat16)
        newr = right_side - jnp.dot(proj.T, left_m, precision=HIGH)
        return newl, newr

    new_left, new_rhs = lax.map(one_tile, (panel_left, panel_right, ranks, rhs))
    pivot_proj = jnp.dot(pivot_wide.T, finished, precision=HIGH)
    pivot_new = pivot_rhs - jnp.dot(pivot_left.astype(jnp.float32), pivot_proj, precision=HIGH)
    next_solution = jnp.dot(diag_inverse, pivot_new, precision=HIGH)
    return new_left, new_rhs, next_solution
```

```python
import jax
import jax.numpy as jnp
from jax import lax
from jax.sharding import PartitionSpec as P

HIGH = lax.Precision.HIGHEST
AXIS = "blk"


def stages_of(count):
    bits = count.bit_length() - 1
    fields = []
    top = bits
    while top > 1:
        width = min(2, top - 1)
        top -= width
        fields.append((top, width))
    if bits:
        fields.append((0, 1))
    return fields


def exchange(block, low, width, count):
    mine = (lax.axis_index(AXIS) >> low) & ((1 << width) - 1)
    parts = [block]
    for step in range(1, 1 << width):
        pairs = [(i, i ^ (step << low)) for i in range(count)]
        parts.append(lax.ppermute(block, AXIS, pairs))
    out = jnp.zeros((1 << width,) + block.shape, block.dtype)
    for step, part in enumerate(parts):
        out = lax.dynamic_update_index_in_dim(out, part, mine ^ step, 0)
    return out


def gather_rows(block, count):
    if count & (count - 1):
        return lax.all_gather(block, AXIS, axis=0, tiled=True)
    fields = stages_of(count)
    out = block
    for low, width in fields:
        out = exchange(out, low, width, count)
    lows = [low for low, _ in fields][::-1]
    order = sorted(range(len(lows)), key=lambda axis: -lows[axis])
    depth = len(lows)
    return out.transpose(tuple(order) + (depth, depth + 1)).reshape(-1, block.shape[-1])


def shards(
    count, panel_left, panel_right, ranks, rhs, pivot_left, pivot_right, finished, pivot_rhs, diag_inverse
):
    kmax = panel_left.shape[1]
    cols = pivot_right.shape[1]
    nrhs = finished.shape[1]
    mask = (jnp.arange(kmax, dtype=jnp.int32)[None, :] < ranks[:, None]).astype(jnp.bfloat16)
    left_m = panel_left * mask[:, :, None]
    right_wide = (panel_right * mask[:, :, None]).astype(jnp.float32)
    mine = jnp.concatenate(
        [pivot_right.astype(jnp.float32), finished, pivot_left.astype(jnp.float32), pivot_rhs], axis=1
    )
    whole = gather_rows(mine, count)
    right_piece = whole[:, :cols]
    solved_piece = whole[:, cols : cols + nrhs]
    left_piece = whole[:, cols + nrhs : 2 * cols + nrhs]
    rhs_piece = whole[:, 2 * cols + nrhs :]
    both = jnp.einsum("rkn,nj->rkj", right_wide, whole[:, : cols + nrhs], precision=HIGH)
    gram_sum = both[:, :, :cols]
    proj_sum = both[:, :, cols:]
    pivot_sum = jnp.dot(right_piece.T, solved_piece, precision=HIGH)
    new_left = jnp.einsum(
        "rkj,rkn->rjn", gram_sum.astype(jnp.bfloat16), left_m, preferred_element_type=jnp.float32
    ).astype(jnp.bfloat16)
    new_rhs = rhs - jnp.einsum("rkj,rkn->rjn", proj_sum, left_m.astype(jnp.float32), precision=HIGH)
    pivot_new = rhs_piece - jnp.dot(left_piece, pivot_sum, precision=HIGH)
    next_solution = jnp.dot(diag_inverse, pivot_new, precision=HIGH)
    return (new_left, new_rhs, next_solution)


def solution(mesh):
    count = mesh.shape[AXIS]
    tile = P(AXIS, None, None)
    row = P(AXIS, None)
    in_specs = (tile, tile, P(AXIS), tile, row, row, row, row, row)

    def local(*args):
        return shards(count, *args)

    return jax.shard_map(local, mesh=mesh, in_specs=in_specs, out_specs=(tile, tile, row), check_vma=False)
```

```python
import functools

import jax
import jax.numpy as jnp
from jax import lax
from jax.experimental import pallas as pl
from jax.experimental.pallas import tpu as pltpu
from jax.sharding import PartitionSpec as P

AXIS = "blk"
F32 = jnp.float32
BF16 = jnp.bfloat16


def fields_of(count):
    bits = count.bit_length() - 1
    fields = []
    top = bits
    while top > 1:
        width = min(2, top - 1)
        top -= width
        fields.append((top, width))
    if bits:
        fields.append((0, 1))
    return fields


def swap(block, mask, count):
    return lax.ppermute(block, AXIS, [(i, i ^ mask) for i in range(count)])


def exchange(block, low, width, count):
    mine = (lax.axis_index(AXIS) >> low) & ((1 << width) - 1)
    parts = [block] + [swap(block, step << low, count) for step in range(1, 1 << width)]
    out = jnp.zeros((1 << width,) + block.shape, block.dtype)
    for step, part in enumerate(parts):
        out = lax.dynamic_update_index_in_dim(out, part, mine ^ step, 0)
    return out


def gather_rows(block, count):
    if count & (count - 1):
        return lax.all_gather(block, AXIS, axis=0, tiled=True)
    fields = fields_of(count)
    out = block
    for low, width in fields:
        out = exchange(out, low, width, count)
    lows = [low for low, _ in fields][::-1]
    order = sorted(range(len(lows)), key=lambda axis: -lows[axis])
    depth = len(lows)
    return out.transpose(tuple(order) + (depth, depth + 1)).reshape(-1, block.shape[-1])


def gather_pieces(block, count):
    rows, width = block.shape
    fields = fields_of(count)
    if count & (count - 1) or rows % 16 or len(fields) != 3:
        return [gather_rows(block, count)[None]], [None]
    first, second, last = fields
    own = exchange(block, *first, count)
    pieces, masks = [], []
    for step in range(1 << second[1]):
        mask = step << second[0]
        piece = swap(own, mask, count) if step else own
        pieces += [piece, swap(piece, 1, count)]
        masks += [mask, mask ^ 1]
    return pieces, masks


def pack_kernel(right, done, left, side, out):
    out[...] = jnp.concatenate(
        [right[...].astype(F32), done[...], left[...].astype(F32), side[...]], axis=1
    )


def split(value):
    high = value.astype(BF16)
    return high, (value - high.astype(F32)).astype(BF16)


def dot(a, b):
    return jnp.dot(a, b, preferred_element_type=F32)


def finish_kernel(masks, stride, ranks, *refs):
    count = len(masks)
    pieces = refs[:count]
    right, left, side, inverse = refs[count : count + 4]
    new_left, new_rhs, solution_out = refs[count + 4 : count + 7]
    both, other, left_buf, rhs_buf, sems = refs[count + 7 :]
    tiles, kmax, _ = left.shape
    wide = both.shape[1] // 2
    half = wide // 2
    me = lax.axis_index(AXIS)
    for piece, mask in zip(pieces, masks):
        groups, rows, _ = piece.shape
        for group in range(groups):
            if mask is None:
                at = group * rows
            else:
                at = pl.multiple_of(((me ^ mask) & (stride - 1)) * rows + group * stride * rows, rows)
            block = piece[group]
            high, low = split(block[:, :wide])
            both[pl.ds(at, rows), :wide] = high
            both[pl.ds(at, rows), wide:] = low
            high, low = split(block[:, wide:])
            other[pl.ds(at, rows), :wide] = high
            other[pl.ds(at, rows), wide:] = low
    flat = right[...].reshape(tiles * kmax, right.shape[2])
    sums = dot(flat, both[...])
    copies = []
    for tile in range(tiles):
        mine = sums[tile * kmax : (tile + 1) * kmax]
        row = lax.broadcasted_iota(jnp.int32, mine.shape, 0)
        mine = jnp.where(row < ranks[tile], mine, 0.0)
        proj = mine[:, half:wide] + mine[:, wide + half :]
        high, low = split(proj)
        weights = jnp.concatenate([mine[:, :half].astype(BF16), high, low], axis=1)
        product = lax.dot_general(
            weights, left[tile], (((0,), (0,)), ((), ())), preferred_element_type=F32
        )
        left_buf[tile] = product[:half].astype(BF16)
        rhs_buf[tile] = side[tile] - (product[half:wide] + product[wide:])
        for buf, hbm, at in ((left_buf, new_left, 0), (rhs_buf, new_rhs, 1)):
            copy = pltpu.make_async_copy(buf.at[tile], hbm.at[tile], sems.at[tile, at])
            copy.start()
            copies.append(copy)
    cross = lax.dot_general(
        both[:, :wide], both[...], (((0,), (0,)), ((), ())), preferred_element_type=F32
    )
    pivot = cross[:half, half:wide] + cross[:half, wide + half :]
    high, low = split(inverse[...])
    rows = high.shape[0]
    solved = dot(jnp.concatenate([high, low], axis=0), other[...])
    left_part = solved[:rows, :half] + solved[rows:, :half]
    rhs_part = solved[:rows, half:wide] + solved[:rows, wide + half :] + solved[rows:, half:wide]
    solution_out[...] = rhs_part - jnp.dot(
        left_part, pivot, precision=lax.Precision.HIGHEST, preferred_element_type=F32
    )
    for copy in copies:
        copy.wait()


def shards(
    count, panel_left, panel_right, ranks, rhs, pivot_left, pivot_right, finished, pivot_rhs, diag_inverse
):
    tiles, kmax, places = panel_left.shape
    rows, cols = pivot_right.shape
    nrhs = finished.shape[1]
    width = 2 * (cols + nrhs)
    vmem = pl.BlockSpec(memory_space=pltpu.VMEM)
    block = pl.pallas_call(
        pack_kernel,
        out_shape=jax.ShapeDtypeStruct((rows, width), F32),
        in_specs=[vmem] * 4,
        out_specs=vmem,
        name="pack",
    )(pivot_right, finished, pivot_left, pivot_rhs)
    pieces, masks = gather_pieces(block, count)
    stride = 1 << fields_of(count)[0][0]
    return pl.pallas_call(
        functools.partial(finish_kernel, masks, stride),
        out_shape=(
            jax.ShapeDtypeStruct(panel_left.shape, BF16),
            jax.ShapeDtypeStruct(rhs.shape, F32),
            jax.ShapeDtypeStruct((rows, nrhs), F32),
        ),
        in_specs=[pl.BlockSpec(memory_space=pltpu.SMEM)] + [vmem] * (len(pieces) + 4),
        out_specs=(pl.BlockSpec(memory_space=pl.ANY), pl.BlockSpec(memory_space=pl.ANY), vmem),
        scratch_shapes=[
            pltpu.VMEM((places, width), BF16),
            pltpu.VMEM((places, width), BF16),
            pltpu.VMEM(panel_left.shape, BF16),
            pltpu.VMEM(rhs.shape, F32),
            pltpu.SemaphoreType.DMA((tiles, 2)),
        ],
        compiler_params=pltpu.CompilerParams(vmem_limit_bytes=24 * 1024 * 1024),
        name="finish",
    )(ranks, *pieces, panel_right, panel_left, rhs, diag_inverse)


def solution(mesh):
    count = mesh.shape[AXIS]
    tile = P(AXIS, None, None)
    row = P(AXIS, None)
    in_specs = (tile, tile, P(AXIS), tile, row, row, row, row, row)

    def local(*args):
        return shards(count, *args)

    return jax.shard_map(local, mesh=mesh, in_specs=in_specs, out_specs=(tile, tile, row), check_vma=False)
```

```python
import functools

import jax
import jax.numpy as jnp
from jax import lax
from jax.experimental import pallas as pl
from jax.experimental.pallas import tpu as pltpu
from jax.sharding import PartitionSpec as P


AXIS = "blk"
PARTS = 2
F32 = jnp.float32
BF16 = jnp.bfloat16
VMEM = pl.BlockSpec(memory_space=pltpu.VMEM)
HBM = pl.BlockSpec(memory_space=pltpu.HBM)


def fields_of(count):
    bits = count.bit_length() - 1
    fields = []
    top = bits
    while top > 1:
        width = min(2, top - 1)
        top -= width
        fields.append((top, width))
    if bits:
        fields.append((0, 1))
    return fields


def swap(block, mask, count):
    return lax.ppermute(block, AXIS, [(i, i ^ mask) for i in range(count)])


def exchange(block, low, width, count):
    mine = (lax.axis_index(AXIS) >> low) & ((1 << width) - 1)
    parts = [block] + [swap(block, step << low, count) for step in range(1, 1 << width)]
    out = jnp.zeros((1 << width,) + block.shape, block.dtype)
    for step, part in enumerate(parts):
        out = lax.dynamic_update_index_in_dim(out, part, mine ^ step, 0)
    return out


def gather_rows(block, count):
    if count & (count - 1):
        return lax.all_gather(block, AXIS, axis=0, tiled=True)
    fields = fields_of(count)
    out = block
    for low, width in fields:
        out = exchange(out, low, width, count)
    lows = [low for low, _ in fields][::-1]
    order = sorted(range(len(lows)), key=lambda axis: -lows[axis])
    depth = len(lows)
    return out.transpose(tuple(order) + (depth, depth + 1)).reshape(-1, block.shape[-1])


def squares(count):
    return not count & (count - 1) and [wide for _, wide in fields_of(count)] == [2, 2, 1]


def gather_halves(block, count):
    _, width = block.shape
    fields = fields_of(count)
    if not squares(count):
        whole = gather_rows(block, count).reshape(2, 1, -1, width)
        return [[(whole[0], None)], [(whole[1], None)]]
    (first, _), (second, _), _ = fields
    steps = [step << first for step in range(4)]
    blocks = [block] + [swap(block, step << first, count) for step in range(1, 4)]
    halves = []
    for at in (0, 2):
        own = jnp.stack(blocks[at : at + 2])
        half = []
        for step in range(4):
            mask = step << second
            piece = swap(own, mask, count) if step else own
            other = swap(piece, 1, count)
            for core, part in ((0, piece), (1, other)):
                half.append((part, [mask ^ core ^ plane for plane in steps[at : at + 2]]))
        halves.append(half)
    return halves


def pack_kernel(right, done, left, side, out, right_buf, done_buf, left_buf, side_buf, sems):
    pairs = ((right, right_buf), (done, done_buf), (left, left_buf), (side, side_buf))
    copies = [pltpu.make_async_copy(hbm, buf, sems.at[at]) for at, (hbm, buf) in enumerate(pairs)]
    for copy in copies:
        copy.start()
    for copy in copies:
        copy.wait()
    out[...] = jnp.concatenate(
        [right_buf[...].astype(F32), done_buf[...], left_buf[...].astype(F32), side_buf[...]], axis=1
    )


def split(value):
    high = value.astype(BF16)
    return high, (value - high.astype(F32)).astype(BF16)


def dot(a, b):
    return jnp.dot(a, b, preferred_element_type=F32)


def dot_rows(a, b):
    return lax.dot_general(a, b, (((0,), (0,)), ((), ())), preferred_element_type=F32)


def start_of(pieces, masks, index, length):
    if masks[0] is None:
        return index * length
    here = (lax.axis_index(AXIS) ^ masks[0][0]) * pieces[0].shape[1]
    return pl.multiple_of(here // length * length, length)


def fill(pieces, masks, buf, offset):
    length, width = buf.shape
    wide = width // 2
    me = lax.axis_index(AXIS)
    for piece, mask in zip(pieces, masks):
        groups, rows, _ = piece.shape
        for group in range(groups):
            at = 0 if mask is None else pl.multiple_of(lax.rem((me ^ mask[group]) * rows, length), rows)
            high, low = split(piece[group, :, offset : offset + wide])
            buf[pl.ds(at, rows), :wide] = high
            buf[pl.ds(at, rows), wide:] = low


def panel_product(pieces, masks, index, right, both):
    length = both.shape[0]
    tiles, kmax, _ = right.shape
    start = start_of(pieces, masks, index, length)
    return dot(right[:, :, pl.ds(start, length)].reshape(tiles * kmax, length), both[...])


def pivot_products(pieces, masks, index, inverse, both, other):
    length, width = both.shape
    start = start_of(pieces, masks, index, length)
    cross = dot_rows(both[:, : width // 4], both[...])
    high, low = split(inverse[:, pl.ds(start, length)])
    return cross, dot(jnp.concatenate([high, low], axis=0), other[...])


def first_kernel(masks, ranks, *refs):
    count = len(masks)
    pieces = refs[:count]
    right, inverse, left, side = refs[count : count + 4]
    sums_out, cross_out, solved_out, keep_out, inverse_out, left_out, side_out = refs[count + 4 : count + 11]
    both, other, sems = refs[count + 11 :]
    pairs = ((inverse, inverse_out), (left, left_out), (side, side_out))
    copies = [pltpu.make_async_copy(hbm, out, sems.at[at]) for at, (hbm, out) in enumerate(pairs)]
    for copy in copies:
        copy.start()
    tiles, kmax, _ = right.shape
    for tile in range(tiles):
        at = pl.ds(tile * kmax, kmax)
        row = lax.broadcasted_iota(jnp.int32, (kmax, keep_out.shape[1]), 0)
        keep_out[at, :] = (row < ranks[tile]).astype(F32)
    fill(pieces, masks, both, 0)
    fill(pieces, masks, other, both.shape[1] // 2)
    sums_out[...] = panel_product(pieces, masks, 0, right, both)
    copies[0].wait()
    cross_out[...], solved_out[...] = pivot_products(pieces, masks, 0, inverse_out, both, other)
    for copy in copies[1:]:
        copy.wait()


def finish_kernel(masks, *refs):
    count = len(masks)
    pieces = refs[:count]
    right, sums_in, cross_in, solved_in, keep, inverse, left, side = refs[count : count + 8]
    new_left, new_rhs, solution_out = refs[count + 8 : count + 11]
    both, other, left_buf, rhs_buf, solution_buf, sems = refs[count + 11 :]
    tiles, kmax, places = left.shape
    wide = both.shape[1] // 2
    half = wide // 2
    fill(pieces, masks, both, 0)
    sums = (panel_product(pieces, masks, 1, right, both) + sums_in[...]) * keep[...]
    fill(pieces, masks, other, wide)
    cross, solved = pivot_products(pieces, masks, 1, inverse, both, other)
    cross += cross_in[...]
    solved += solved_in[...]
    high, low = split(cross[:, half:wide] + cross[:, wide + half :])
    pivot = jnp.concatenate([high, low, high], axis=0)
    rows = solved.shape[0] // 2
    high, low = split(solved[:rows, :half] + solved[rows:, :half])
    rhs_part = solved[:rows, half:wide] + solved[:rows, wide + half :] + solved[rows:, half:wide]
    solution_buf[...] = rhs_part - dot(jnp.concatenate([high, high, low], axis=1), pivot)
    last = pltpu.make_async_copy(solution_buf, solution_out, sems.at[2 * PARTS * tiles])
    last.start()
    copies = []
    span = places // PARTS
    for tile in range(tiles):
        mine = sums[tile * kmax : (tile + 1) * kmax]
        high, low = split(mine[:, half:wide] + mine[:, wide + half :])
        weights = jnp.concatenate([mine[:, :half].astype(BF16), high, low], axis=1)
        for part in range(PARTS):
            at = (tile, slice(None), pl.ds(part * span, span))
            product = dot_rows(weights, left[at])
            left_buf[at] = product[:half].astype(BF16)
            rhs_buf[at] = side[at] - (product[half:wide] + product[wide:])
            for buf, hbm in ((left_buf, new_left), (rhs_buf, new_rhs)):
                copy = pltpu.make_async_copy(buf.at[at], hbm.at[at], sems.at[len(copies)])
                copy.start()
                copies.append(copy)

    for copy in copies + [last]:
        copy.wait()


def shards(
    count, panel_left, panel_right, ranks, rhs, pivot_left, pivot_right, finished, pivot_rhs, diag_inverse
):
    tiles, kmax, places = panel_left.shape
    rows, cols = pivot_right.shape
    nrhs = finished.shape[1]
    width = 2 * (cols + nrhs)
    params = pltpu.CompilerParams(vmem_limit_bytes=20 * 1024 * 1024)
    first_params = pltpu.CompilerParams(vmem_limit_bytes=52_000_000)
    block = pl.pallas_call(
        pack_kernel,
        out_shape=pltpu.VMEM((rows, width), F32),
        in_specs=[HBM] * 4,
        out_specs=VMEM,
        scratch_shapes=[
            pltpu.VMEM((rows, cols), BF16),
            pltpu.VMEM((rows, nrhs), F32),
            pltpu.VMEM((rows, cols), BF16),
            pltpu.VMEM((rows, nrhs), F32),
            pltpu.SemaphoreType.DMA((4,)),
        ],
        name="pack",
    )(pivot_right, finished, pivot_left, pivot_rhs)
    near, far = gather_halves(block, count)
    halves = [pltpu.VMEM((places // 2, width), BF16)] * 2
    middle = pl.pallas_call(
        functools.partial(first_kernel, [mask for _, mask in near]),
        out_shape=(
            pltpu.VMEM((tiles * kmax, width), F32),
            pltpu.VMEM((cols, width), F32),
            pltpu.VMEM((2 * rows, width), F32),
            pltpu.VMEM((tiles * kmax, width), F32),
            pltpu.VMEM(diag_inverse.shape, F32),
            pltpu.VMEM(panel_left.shape, BF16),
            pltpu.VMEM(rhs.shape, F32),
        ),
        in_specs=[pl.BlockSpec(memory_space=pltpu.SMEM)] + [VMEM] * (len(near) + 1) + [HBM] * 3,
        out_specs=(VMEM,) * 7,
        scratch_shapes=halves + [pltpu.SemaphoreType.DMA((3,))],
        compiler_params=first_params,
        cost_estimate=pl.CostEstimate(flops=300_000_000, bytes_accessed=4_000_000, transcendentals=0),
        name="first",
    )(ranks, *[piece for piece, _ in near], panel_right, diag_inverse, panel_left, rhs)
    return pl.pallas_call(
        functools.partial(finish_kernel, [mask for _, mask in far]),
        out_shape=(
            jax.ShapeDtypeStruct(panel_left.shape, BF16),
            jax.ShapeDtypeStruct(rhs.shape, F32),
            jax.ShapeDtypeStruct((rows, nrhs), F32),
        ),
        in_specs=[VMEM] * (len(far) + 8),
        out_specs=(HBM,) * 3,
        scratch_shapes=halves
        + [
            pltpu.VMEM(panel_left.shape, BF16),
            pltpu.VMEM(rhs.shape, F32),
            pltpu.VMEM((rows, nrhs), F32),
            pltpu.SemaphoreType.DMA((2 * PARTS * tiles + 1,)),
        ],
        compiler_params=params,
        name="finish",
    )(*[piece for piece, _ in far], panel_right, *middle)


def solution(mesh):
    count = mesh.shape[AXIS]
    tile = P(AXIS, None, None)
    row = P(AXIS, None)
    in_specs = (tile, tile, P(AXIS), tile, row, row, row, row, row)

    def local(*args):
        return shards(count, *args)

    step = jax.shard_map(local, mesh=mesh, in_specs=in_specs, out_specs=(tile, tile, row), check_vma=False)
    return step if squares(count) else step
```

```python
import functools

import jax
import jax.numpy as jnp
from jax import lax
from jax.experimental import pallas as pl
from jax.experimental.pallas import tpu as pltpu
from jax.sharding import PartitionSpec as P


AXIS = "blk"
PARTS = 1
F32 = jnp.float32
BF16 = jnp.bfloat16
VMEM = pl.BlockSpec(memory_space=pltpu.VMEM)
HBM = pl.BlockSpec(memory_space=pltpu.HBM)


def fields_of(count):
    bits = count.bit_length() - 1
    fields = []
    top = bits
    while top > 1:
        width = min(2, top - 1)
        top -= width
        fields.append((top, width))
    if bits:
        fields.append((0, 1))
    return fields


def swap(block, mask, count):
    return lax.ppermute(block, AXIS, [(i, i ^ mask) for i in range(count)])


def exchange(block, low, width, count):
    mine = (lax.axis_index(AXIS) >> low) & ((1 << width) - 1)
    parts = [block] + [swap(block, step << low, count) for step in range(1, 1 << width)]
    out = jnp.zeros((1 << width,) + block.shape, block.dtype)
    for step, part in enumerate(parts):
        out = lax.dynamic_update_index_in_dim(out, part, mine ^ step, 0)
    return out


def gather_rows(block, count):
    if count & (count - 1):
        return lax.all_gather(block, AXIS, axis=0, tiled=True)
    fields = fields_of(count)
    out = block
    for low, width in fields:
        out = exchange(out, low, width, count)
    lows = [low for low, _ in fields][::-1]
    order = sorted(range(len(lows)), key=lambda axis: -lows[axis])
    depth = len(lows)
    return out.transpose(tuple(order) + (depth, depth + 1)).reshape(-1, block.shape[-1])


def squares(count):
    return not count & (count - 1) and [wide for _, wide in fields_of(count)] == [2, 2, 1]


def gather_halves(block, count):
    _, width = block.shape
    fields = fields_of(count)
    if not squares(count):
        whole = gather_rows(block, count).reshape(2, 1, -1, width)
        return [[(whole[0], None)], [(whole[1], None)]]
    (first, _), (second, _), _ = fields
    steps = [step << first for step in range(4)]
    blocks = [block] + [swap(block, step << first, count) for step in range(1, 4)]
    halves = []
    for at in (0, 2):
        own = jnp.stack(blocks[at : at + 2])
        half = []
        for step in range(4):
            mask = step << second
            piece = swap(own, mask, count) if step else own
            other = swap(piece, 1, count)
            for core, part in ((0, piece), (1, other)):
                half.append((part, [mask ^ core ^ plane for plane in steps[at : at + 2]]))
        halves.append(half)
    return halves


def pack_kernel(right, done, left, side, out, right_buf, done_buf, left_buf, side_buf, sems):
    pairs = ((right, right_buf), (done, done_buf), (left, left_buf), (side, side_buf))
    copies = [pltpu.make_async_copy(hbm, buf, sems.at[at]) for at, (hbm, buf) in enumerate(pairs)]
    for copy in copies:
        copy.start()
    for copy in copies:
        copy.wait()
    out[...] = jnp.concatenate(
        [right_buf[...].astype(F32), done_buf[...], left_buf[...].astype(F32), side_buf[...]], axis=1
    )


def split(value):
    high = value.astype(BF16)
    return high, (value - high.astype(F32)).astype(BF16)


def dot(a, b):
    return jnp.dot(a, b, preferred_element_type=F32)


def dot_rows(a, b):
    return lax.dot_general(a, b, (((0,), (0,)), ((), ())), preferred_element_type=F32)


def start_of(pieces, masks, index, length):
    if masks[0] is None:
        return index * length
    here = (lax.axis_index(AXIS) ^ masks[0][0]) * pieces[0].shape[1]
    return pl.multiple_of(here // length * length, length)


def fill(pieces, masks, buf, offset):
    length, width = buf.shape
    wide = width // 2
    me = lax.axis_index(AXIS)
    for piece, mask in zip(pieces, masks):
        groups, rows, _ = piece.shape
        for group in range(groups):
            at = 0 if mask is None else pl.multiple_of(lax.rem((me ^ mask[group]) * rows, length), rows)
            high, low = split(piece[group, :, offset : offset + wide])
            buf[pl.ds(at, rows), :wide] = high
            buf[pl.ds(at, rows), wide:] = low


def panel_product(pieces, masks, index, right, both):
    length = both.shape[0]
    tiles, kmax, _ = right.shape
    start = start_of(pieces, masks, index, length)
    return dot(right[:, :, pl.ds(start, length)].reshape(tiles * kmax, length), both[...])


def pivot_products(pieces, masks, index, inverse, both, other):
    length, width = both.shape
    start = start_of(pieces, masks, index, length)
    cross = dot_rows(both[:, : width // 4], both[...])
    high, low = split(inverse[:, pl.ds(start, length)])
    return cross, dot(jnp.concatenate([high, low], axis=0), other[...])


def load_kernel(kmax, ranks, inverse, left, side, keep, inverse_out, left_out, side_out, sems):
    pairs = ((inverse, inverse_out), (left, left_out), (side, side_out))
    copies = [pltpu.make_async_copy(hbm, out, sems.at[at]) for at, (hbm, out) in enumerate(pairs)]
    for copy in copies:
        copy.start()
    for tile in range(keep.shape[0] // kmax):
        row = lax.broadcasted_iota(jnp.int32, (kmax, keep.shape[1]), 0)
        keep[pl.ds(tile * kmax, kmax), :] = (row < ranks[tile]).astype(F32)
    for copy in copies:
        copy.wait()


def first_kernel(masks, *refs):
    count = len(masks)
    pieces = refs[:count]
    right, inverse, sums_out, cross_out, solved_out, both, other = refs[count:]
    fill(pieces, masks, both, 0)
    fill(pieces, masks, other, both.shape[1] // 2)
    sums_out[...] = panel_product(pieces, masks, 0, right, both)
    cross_out[...], solved_out[...] = pivot_products(pieces, masks, 0, inverse, both, other)


def finish_kernel(masks, *refs):
    count = len(masks)
    pieces = refs[:count]
    right, keep, sums_in, cross_in, solved_in, inverse, left, side = refs[count : count + 8]
    new_left, new_rhs, solution_out = refs[count + 8 : count + 11]
    both, other, left_buf, rhs_buf, solution_buf, sems = refs[count + 11 :]
    tiles, kmax, places = left.shape
    wide = both.shape[1] // 2
    half = wide // 2
    fill(pieces, masks, both, 0)
    sums = (panel_product(pieces, masks, 1, right, both) + sums_in[...]) * keep[...]
    fill(pieces, masks, other, wide)
    cross, solved = pivot_products(pieces, masks, 1, inverse, both, other)
    cross += cross_in[...]
    solved += solved_in[...]
    high, low = split(cross[:, half:wide] + cross[:, wide + half :])
    pivot = jnp.concatenate([high, low, high], axis=0)
    rows = solved.shape[0] // 2
    high, low = split(solved[:rows, :half] + solved[rows:, :half])
    rhs_part = solved[:rows, half:wide] + solved[:rows, wide + half :] + solved[rows:, half:wide]
    solution_buf[...] = rhs_part - dot(jnp.concatenate([high, high, low], axis=1), pivot)
    last = pltpu.make_async_copy(solution_buf, solution_out, sems.at[2 * PARTS * tiles])
    last.start()
    copies = []
    span = places // PARTS
    for tile in range(tiles):
        mine = sums[tile * kmax : (tile + 1) * kmax]
        high, low = split(mine[:, half:wide] + mine[:, wide + half :])
        gram = mine[:, :half].astype(BF16)
        weights = jnp.concatenate(
            [
                jnp.concatenate([gram, high], axis=1),
                jnp.concatenate([jnp.zeros_like(gram), low], axis=1),
            ],
            axis=0,
        )
        for part in range(PARTS):
            at = (tile, slice(None), pl.ds(part * span, span))
            product = dot_rows(weights, jnp.concatenate([left[at], left[at]], axis=0))
            left_buf[at] = product[:half].astype(BF16)
            rhs_buf[at] = side[at] - product[half:]
            for buf, hbm in ((left_buf, new_left), (rhs_buf, new_rhs)):
                copy = pltpu.make_async_copy(buf.at[at], hbm.at[at], sems.at[len(copies)])
                copy.start()
                copies.append(copy)

    for copy in copies + [last]:
        copy.wait()


def shards(
    count, panel_left, panel_right, ranks, rhs, pivot_left, pivot_right, finished, pivot_rhs, diag_inverse
):
    tiles, kmax, places = panel_left.shape
    rows, cols = pivot_right.shape
    nrhs = finished.shape[1]
    width = 2 * (cols + nrhs)
    params = pltpu.CompilerParams(vmem_limit_bytes=20 * 1024 * 1024)
    load_params = pltpu.CompilerParams(vmem_limit_bytes=56_000_000)
    block = pl.pallas_call(
        pack_kernel,
        out_shape=pltpu.VMEM((rows, width), F32),
        in_specs=[HBM] * 4,
        out_specs=VMEM,
        scratch_shapes=[
            pltpu.VMEM((rows, cols), BF16),
            pltpu.VMEM((rows, nrhs), F32),
            pltpu.VMEM((rows, cols), BF16),
            pltpu.VMEM((rows, nrhs), F32),
            pltpu.SemaphoreType.DMA((4,)),
        ],
        name="pack",
    )(pivot_right, finished, pivot_left, pivot_rhs)
    near, far = gather_halves(block, count)
    keep, inverse, left, side = pl.pallas_call(
        functools.partial(load_kernel, kmax),
        out_shape=(
            pltpu.VMEM((tiles * kmax, width), F32),
            pltpu.VMEM(diag_inverse.shape, F32),
            pltpu.VMEM(panel_left.shape, BF16),
            pltpu.VMEM(rhs.shape, F32),
        ),
        in_specs=[pl.BlockSpec(memory_space=pltpu.SMEM)] + [HBM] * 3,
        out_specs=(VMEM,) * 4,
        scratch_shapes=[pltpu.SemaphoreType.DMA((3,))],
        compiler_params=load_params,
        name="load",
    )(ranks, diag_inverse, panel_left, rhs)
    halves = [pltpu.VMEM((places // 2, width), BF16)] * 2
    middle = pl.pallas_call(
        functools.partial(first_kernel, [mask for _, mask in near]),
        out_shape=(
            pltpu.VMEM((tiles * kmax, width), F32),
            pltpu.VMEM((cols, width), F32),
            pltpu.VMEM((2 * rows, width), F32),
        ),
        in_specs=[VMEM] * (len(near) + 2),
        out_specs=(VMEM,) * 3,
        scratch_shapes=halves,
        compiler_params=params,
        cost_estimate=pl.CostEstimate(flops=300_000_000, bytes_accessed=4_000_000, transcendentals=0),
        name="first",
    )(*[piece for piece, _ in near], panel_right, inverse)
    return pl.pallas_call(
        functools.partial(finish_kernel, [mask for _, mask in far]),
        out_shape=(
            jax.ShapeDtypeStruct(panel_left.shape, BF16),
            jax.ShapeDtypeStruct(rhs.shape, F32),
            jax.ShapeDtypeStruct((rows, nrhs), F32),
        ),
        in_specs=[VMEM] * (len(far) + 8),
        out_specs=(HBM,) * 3,
        scratch_shapes=halves
        + [
            pltpu.VMEM(panel_left.shape, BF16),
            pltpu.VMEM(rhs.shape, F32),
            pltpu.VMEM((rows, nrhs), F32),
            pltpu.SemaphoreType.DMA((2 * PARTS * tiles + 1,)),
        ],
        compiler_params=params,
        name="finish",
    )(*[piece for piece, _ in far], panel_right, keep, *middle, inverse, left, side)


def solution(mesh):
    count = mesh.shape[AXIS]
    tile = P(AXIS, None, None)
    row = P(AXIS, None)
    in_specs = (tile, tile, P(AXIS), tile, row, row, row, row, row)

    def local(*args):
        return shards(count, *args)

    step = jax.shard_map(local, mesh=mesh, in_specs=in_specs, out_specs=(tile, tile, row), check_vma=False)
    return step if squares(count) else step
```

```python
import functools

import jax
import jax.numpy as jnp
from jax import lax
from jax.experimental import pallas as pl
from jax.experimental.pallas import tpu as pltpu
from jax.sharding import PartitionSpec as P


AXIS = "blk"
PARTS = 1
CORE_GROUPS = {"near": [[3, 2, 1, 0]], "far": [[0, 3], [2, 1]]}
F32 = jnp.float32
BF16 = jnp.bfloat16
VMEM = pl.BlockSpec(memory_space=pltpu.VMEM)
HBM = pl.BlockSpec(memory_space=pltpu.HBM)


def fields_of(count):
    bits = count.bit_length() - 1
    fields = []
    top = bits
    while top > 1:
        width = min(2, top - 1)
        top -= width
        fields.append((top, width))
    if bits:
        fields.append((0, 1))
    return fields


def swap(block, mask, count):
    return lax.ppermute(block, AXIS, [(i, i ^ mask) for i in range(count)])


def exchange(block, low, width, count):
    mine = (lax.axis_index(AXIS) >> low) & ((1 << width) - 1)
    parts = [block] + [swap(block, step << low, count) for step in range(1, 1 << width)]
    out = jnp.zeros((1 << width,) + block.shape, block.dtype)
    for step, part in enumerate(parts):
        out = lax.dynamic_update_index_in_dim(out, part, mine ^ step, 0)
    return out


def gather_rows(block, count):
    if count & (count - 1):
        return lax.all_gather(block, AXIS, axis=0, tiled=True)
    fields = fields_of(count)
    out = block
    for low, width in fields:
        out = exchange(out, low, width, count)
    lows = [low for low, _ in fields][::-1]
    order = sorted(range(len(lows)), key=lambda axis: -lows[axis])
    depth = len(lows)
    return out.transpose(tuple(order) + (depth, depth + 1)).reshape(-1, block.shape[-1])


def squares(count):
    return not count & (count - 1) and [wide for _, wide in fields_of(count)] == [2, 2, 1]


def gather_halves(block, count):
    _, width = block.shape
    fields = fields_of(count)
    if not squares(count):
        whole = gather_rows(block, count).reshape(2, 1, -1, width)
        return [[(whole[0], None)], [(whole[1], None)]]
    (first, _), (second, _), _ = fields
    steps = [step << first for step in range(4)]
    blocks = [block] + [swap(block, step << first, count) for step in range(1, 4)]
    halves = []
    for at, name in ((0, "near"), (2, "far")):
        own = jnp.stack(blocks[at : at + 2])
        parts = [own] + [swap(own, step << second, count) for step in range(1, 4)]
        masks = [[step << second ^ plane for plane in steps[at : at + 2]] for step in range(4)]
        half = list(zip(parts, masks))
        for group in CORE_GROUPS[name]:
            sent = jnp.concatenate([parts[step] for step in group])
            mask = [value ^ 1 for step in group for value in masks[step]]
            half.append((swap(sent, 1, count), mask))
        halves.append(half)
    return halves


def pack_kernel(right, done, left, side, out, right_buf, done_buf, left_buf, side_buf, sems):
    pairs = ((right, right_buf), (done, done_buf), (left, left_buf), (side, side_buf))
    copies = [pltpu.make_async_copy(hbm, buf, sems.at[at]) for at, (hbm, buf) in enumerate(pairs)]
    for copy in copies:
        copy.start()
    for copy in copies:
        copy.wait()
    out[...] = jnp.concatenate(
        [right_buf[...].astype(F32), done_buf[...], left_buf[...].astype(F32), side_buf[...]], axis=1
    )


def split(value):
    high = value.astype(BF16)
    return high, (value - high.astype(F32)).astype(BF16)


def dot(a, b):
    return jnp.dot(a, b, preferred_element_type=F32)


def dot_rows(a, b):
    return lax.dot_general(a, b, (((0,), (0,)), ((), ())), preferred_element_type=F32)


def start_of(pieces, masks, index, length):
    if masks[0] is None:
        return index * length
    here = (lax.axis_index(AXIS) ^ masks[0][0]) * pieces[0].shape[1]
    return pl.multiple_of(here // length * length, length)


def fill(pieces, masks, buf, offset):
    length, width = buf.shape
    wide = width // 2
    me = lax.axis_index(AXIS)
    for piece, mask in zip(pieces, masks):
        groups, rows, _ = piece.shape
        for group in range(groups):
            at = 0 if mask is None else pl.multiple_of(lax.rem((me ^ mask[group]) * rows, length), rows)
            high, low = split(piece[group, :, offset : offset + wide])
            buf[pl.ds(at, rows), :wide] = high
            buf[pl.ds(at, rows), wide:] = low


def panel_product(pieces, masks, index, right, both):
    length = both.shape[0]
    tiles, kmax, _ = right.shape
    start = start_of(pieces, masks, index, length)
    return dot(right[:, :, pl.ds(start, length)].reshape(tiles * kmax, length), both[...])


def pivot_products(pieces, masks, index, inverse, both, other):
    length, width = both.shape
    start = start_of(pieces, masks, index, length)
    cross = dot_rows(both[:, : width // 4], both[...])
    high, low = split(inverse[:, pl.ds(start, length)])
    return cross, dot(jnp.concatenate([high, low], axis=0), other[...])


def load_kernel(kmax, ranks, inverse, left, side, keep, inverse_out, left_out, side_out, sems):
    pairs = ((inverse, inverse_out), (left, left_out), (side, side_out))
    copies = [pltpu.make_async_copy(hbm, out, sems.at[at]) for at, (hbm, out) in enumerate(pairs)]
    for copy in copies:
        copy.start()
    for tile in range(keep.shape[0] // kmax):
        row = lax.broadcasted_iota(jnp.int32, (kmax, keep.shape[1]), 0)
        keep[pl.ds(tile * kmax, kmax), :] = (row < ranks[tile]).astype(F32)
    for copy in copies:
        copy.wait()


def first_kernel(masks, *refs):
    count = len(masks)
    pieces = refs[:count]
    right, inverse, sums_out, cross_out, solved_out, both, other = refs[count:]
    fill(pieces, masks, both, 0)
    fill(pieces, masks, other, both.shape[1] // 2)
    sums_out[...] = panel_product(pieces, masks, 0, right, both)
    cross_out[...], solved_out[...] = pivot_products(pieces, masks, 0, inverse, both, other)


def finish_kernel(masks, *refs):
    count = len(masks)
    pieces = refs[:count]
    right, keep, sums_in, cross_in, solved_in, inverse, left, side = refs[count : count + 8]
    new_left, new_rhs, solution_out = refs[count + 8 : count + 11]
    both, other, left_buf, rhs_buf, solution_buf, sems = refs[count + 11 :]
    tiles, kmax, places = left.shape
    wide = both.shape[1] // 2
    half = wide // 2
    fill(pieces, masks, both, 0)
    sums = (panel_product(pieces, masks, 1, right, both) + sums_in[...]) * keep[...]
    fill(pieces, masks, other, wide)
    cross, solved = pivot_products(pieces, masks, 1, inverse, both, other)
    cross += cross_in[...]
    solved += solved_in[...]
    high, low = split(cross[:, half:wide] + cross[:, wide + half :])
    pivot = jnp.concatenate([high, low, high], axis=0)
    rows = solved.shape[0] // 2
    high, low = split(solved[:rows, :half] + solved[rows:, :half])
    rhs_part = solved[:rows, half:wide] + solved[:rows, wide + half :] + solved[rows:, half:wide]
    solution_buf[...] = rhs_part - dot(jnp.concatenate([high, high, low], axis=1), pivot)
    last = pltpu.make_async_copy(solution_buf, solution_out, sems.at[2 * PARTS * tiles])
    last.start()
    copies = []
    span = places // PARTS
    for tile in range(tiles):
        mine = sums[tile * kmax : (tile + 1) * kmax]
        high, low = split(mine[:, half:wide] + mine[:, wide + half :])
        gram = mine[:, :half].astype(BF16)
        weights = jnp.concatenate(
            [
                jnp.concatenate([gram, high], axis=1),
                jnp.concatenate([jnp.zeros_like(gram), low], axis=1),
            ],
            axis=0,
        )
        for part in range(PARTS):
            at = (tile, slice(None), pl.ds(part * span, span))
            product = dot_rows(weights, jnp.concatenate([left[at], left[at]], axis=0))
            left_buf[at] = product[:half].astype(BF16)
            rhs_buf[at] = side[at] - product[half:]
            for buf, hbm in ((left_buf, new_left), (rhs_buf, new_rhs)):
                copy = pltpu.make_async_copy(buf.at[at], hbm.at[at], sems.at[len(copies)])
                copy.start()
                copies.append(copy)

    for copy in copies + [last]:
        copy.wait()


def shards(
    count, panel_left, panel_right, ranks, rhs, pivot_left, pivot_right, finished, pivot_rhs, diag_inverse
):
    tiles, kmax, places = panel_left.shape
    rows, cols = pivot_right.shape
    nrhs = finished.shape[1]
    width = 2 * (cols + nrhs)
    params = pltpu.CompilerParams(vmem_limit_bytes=20 * 1024 * 1024)
    load_params = pltpu.CompilerParams(vmem_limit_bytes=56_000_000)
    block = pl.pallas_call(
        pack_kernel,
        out_shape=pltpu.VMEM((rows, width), F32),
        in_specs=[HBM] * 4,
        out_specs=VMEM,
        scratch_shapes=[
            pltpu.VMEM((rows, cols), BF16),
            pltpu.VMEM((rows, nrhs), F32),
            pltpu.VMEM((rows, cols), BF16),
            pltpu.VMEM((rows, nrhs), F32),
            pltpu.SemaphoreType.DMA((4,)),
        ],
        name="pack",
    )(pivot_right, finished, pivot_left, pivot_rhs)
    near, far = gather_halves(block, count)
    keep, inverse, left, side = pl.pallas_call(
        functools.partial(load_kernel, kmax),
        out_shape=(
            pltpu.VMEM((tiles * kmax, width), F32),
            pltpu.VMEM(diag_inverse.shape, F32),
            pltpu.VMEM(panel_left.shape, BF16),
            pltpu.VMEM(rhs.shape, F32),
        ),
        in_specs=[pl.BlockSpec(memory_space=pltpu.SMEM)] + [HBM] * 3,
        out_specs=(VMEM,) * 4,
        scratch_shapes=[pltpu.SemaphoreType.DMA((3,))],
        compiler_params=load_params,
        name="load",
    )(ranks, diag_inverse, panel_left, rhs)
    halves = [pltpu.VMEM((places // 2, width), BF16)] * 2
    middle = pl.pallas_call(
        functools.partial(first_kernel, [mask for _, mask in near]),
        out_shape=(
            pltpu.VMEM((tiles * kmax, width), F32),
            pltpu.VMEM((cols, width), F32),
            pltpu.VMEM((2 * rows, width), F32),
        ),
        in_specs=[VMEM] * (len(near) + 2),
        out_specs=(VMEM,) * 3,
        scratch_shapes=halves,
        compiler_params=params,
        cost_estimate=pl.CostEstimate(flops=300_000_000, bytes_accessed=4_000_000, transcendentals=0),
        name="first",
    )(*[piece for piece, _ in near], panel_right, inverse)
    return pl.pallas_call(
        functools.partial(finish_kernel, [mask for _, mask in far]),
        out_shape=(
            jax.ShapeDtypeStruct(panel_left.shape, BF16),
            jax.ShapeDtypeStruct(rhs.shape, F32),
            jax.ShapeDtypeStruct((rows, nrhs), F32),
        ),
        in_specs=[VMEM] * (len(far) + 8),
        out_specs=(HBM,) * 3,
        scratch_shapes=halves
        + [
            pltpu.VMEM(panel_left.shape, BF16),
            pltpu.VMEM(rhs.shape, F32),
            pltpu.VMEM((rows, nrhs), F32),
            pltpu.SemaphoreType.DMA((2 * PARTS * tiles + 1,)),
        ],
        compiler_params=params,
        name="finish",
    )(*[piece for piece, _ in far], panel_right, keep, *middle, inverse, left, side)


def solution(mesh):
    count = mesh.shape[AXIS]
    tile = P(AXIS, None, None)
    row = P(AXIS, None)
    in_specs = (tile, tile, P(AXIS), tile, row, row, row, row, row)

    def local(*args):
        return shards(count, *args)

    step = jax.shard_map(local, mesh=mesh, in_specs=in_specs, out_specs=(tile, tile, row), check_vma=False)
    return step if squares(count) else step
```

```python
import functools

import jax
import jax.numpy as jnp
from jax import lax
from jax.experimental import pallas as pl
from jax.experimental.pallas import tpu as pltpu
from jax.sharding import PartitionSpec as P


AXIS = "blk"
PARTS = 1
CORE_GROUPS = {"near": [[3, 2, 1, 0]], "far": [[0, 3], [2, 1]]}
F32 = jnp.float32
BF16 = jnp.bfloat16
VMEM = pl.BlockSpec(memory_space=pltpu.VMEM)
HBM = pl.BlockSpec(memory_space=pltpu.HBM)


def fields_of(count):
    bits = count.bit_length() - 1
    fields = []
    top = bits
    while top > 1:
        width = min(2, top - 1)
        top -= width
        fields.append((top, width))
    if bits:
        fields.append((0, 1))
    return fields


def swap(block, mask, count):
    return lax.ppermute(block, AXIS, [(i, i ^ mask) for i in range(count)])


def exchange(block, low, width, count):
    mine = (lax.axis_index(AXIS) >> low) & ((1 << width) - 1)
    parts = [block] + [swap(block, step << low, count) for step in range(1, 1 << width)]
    out = jnp.zeros((1 << width,) + block.shape, block.dtype)
    for step, part in enumerate(parts):
        out = lax.dynamic_update_index_in_dim(out, part, mine ^ step, 0)
    return out


def gather_rows(block, count):
    if count & (count - 1):
        return lax.all_gather(block, AXIS, axis=0, tiled=True)
    fields = fields_of(count)
    out = block
    for low, width in fields:
        out = exchange(out, low, width, count)
    lows = [low for low, _ in fields][::-1]
    order = sorted(range(len(lows)), key=lambda axis: -lows[axis])
    depth = len(lows)
    return out.transpose(tuple(order) + (depth, depth + 1)).reshape(-1, block.shape[-1])


def squares(count):
    return not count & (count - 1) and [wide for _, wide in fields_of(count)] == [2, 2, 1]


def gather_halves(block, count):
    _, width = block.shape
    fields = fields_of(count)
    if not squares(count):
        whole = gather_rows(block, count).reshape(2, 1, -1, width)
        return [[(whole[0], None)], [(whole[1], None)]]
    (first, _), (second, _), _ = fields
    steps = [step << first for step in range(4)]
    blocks = [block] + [swap(block, step << first, count) for step in range(1, 4)]
    halves = []
    for at, name in ((0, "near"), (2, "far")):
        own = jnp.stack(blocks[at : at + 2])
        parts = [own] + [swap(own, step << second, count) for step in range(1, 4)]
        masks = [[step << second ^ plane for plane in steps[at : at + 2]] for step in range(4)]
        half = list(zip(parts, masks))
        for group in CORE_GROUPS[name]:
            sent = jnp.concatenate([parts[step] for step in group])
            mask = [value ^ 1 for step in group for value in masks[step]]
            half.append((swap(sent, 1, count), mask))
        halves.append(half)
    return halves


def pack_kernel(right, done, left, side, out, right_buf, done_buf, left_buf, side_buf, sems):
    pairs = ((right, right_buf), (done, done_buf), (left, left_buf), (side, side_buf))
    copies = [pltpu.make_async_copy(hbm, buf, sems.at[at]) for at, (hbm, buf) in enumerate(pairs)]
    for copy in copies:
        copy.start()
    for copy in copies:
        copy.wait()
    out[...] = jnp.concatenate(
        [right_buf[...].astype(F32), done_buf[...], left_buf[...].astype(F32), side_buf[...]], axis=1
    )


def split(value):
    high = value.astype(BF16)
    return high, (value - high.astype(F32)).astype(BF16)


def dot(a, b):
    return jnp.dot(a, b, preferred_element_type=F32)


def dot_rows(a, b):
    return lax.dot_general(a, b, (((0,), (0,)), ((), ())), preferred_element_type=F32)


def start_of(pieces, masks, index, length):
    if masks[0] is None:
        return index * length
    here = (lax.axis_index(AXIS) ^ masks[0][0]) * pieces[0].shape[1]
    return pl.multiple_of(here // length * length, length)


def fill(pieces, masks, buf, offset):
    length, width = buf.shape
    wide = width // 2
    me = lax.axis_index(AXIS)
    for piece, mask in zip(pieces, masks):
        groups, rows, _ = piece.shape
        for group in range(groups):
            at = 0 if mask is None else pl.multiple_of(lax.rem((me ^ mask[group]) * rows, length), rows)
            high, low = split(piece[group, :, offset : offset + wide])
            buf[pl.ds(at, rows), :wide] = high
            buf[pl.ds(at, rows), wide:] = low


def panel_product(pieces, masks, index, right, both):
    length = both.shape[0]
    tiles, kmax, _ = right.shape
    start = start_of(pieces, masks, index, length)
    return dot(right[:, :, pl.ds(start, length)].reshape(tiles * kmax, length), both[...])


def stacked(inverse, start, length):
    high, low = split(inverse[:, pl.ds(pl.multiple_of(start, length), length)])
    return jnp.concatenate([high, low], axis=0)


def pivot_products(both, other, inverse):
    return dot_rows(both[:, : both.shape[1] // 4], both[...]), dot(inverse, other[...])


def load_kernel(kmax, ranks, inverse, left, side, keep, inverse_out, left_out, side_out, sems):
    pairs = ((inverse, inverse_out), (left, left_out), (side, side_out))
    copies = [pltpu.make_async_copy(hbm, out, sems.at[at]) for at, (hbm, out) in enumerate(pairs)]
    for copy in copies:
        copy.start()
    for tile in range(keep.shape[0] // kmax):
        row = lax.broadcasted_iota(jnp.int32, (kmax, keep.shape[1]), 0)
        keep[pl.ds(tile * kmax, kmax), :] = (row < ranks[tile]).astype(F32)
    for copy in copies:
        copy.wait()


def first_kernel(masks, *refs):
    count = len(masks)
    pieces = refs[:count]
    right, inverse, sums_out, cross_out, solved_out, far_out, both, other = refs[count:]
    fill(pieces, masks, both, 0)
    fill(pieces, masks, other, both.shape[1] // 2)
    sums_out[...] = panel_product(pieces, masks, 0, right, both)
    length = both.shape[0]
    start = start_of(pieces, masks, 0, length)
    cross_out[...], solved_out[...] = pivot_products(both, other, stacked(inverse, start, length))
    far_out[...] = stacked(inverse, inverse.shape[1] - length - start, length)


def finish_kernel(masks, *refs):
    count = len(masks)
    pieces = refs[:count]
    right, keep, sums_in, cross_in, solved_in, inverse, left, side = refs[count : count + 8]
    new_left, new_rhs, solution_out = refs[count + 8 : count + 11]
    both, other, left_buf, rhs_buf, solution_buf, sems = refs[count + 11 :]
    tiles, kmax, places = left.shape
    wide = both.shape[1] // 2
    half = wide // 2
    fill(pieces, masks, both, 0)
    sums = (panel_product(pieces, masks, 1, right, both) + sums_in[...]) * keep[...]
    fill(pieces, masks, other, wide)
    cross, solved = pivot_products(both, other, inverse[...])
    cross += cross_in[...]
    solved += solved_in[...]
    high, low = split(cross[:, half:wide] + cross[:, wide + half :])
    pivot = jnp.concatenate([high, low, high], axis=0)
    rows = solved.shape[0] // 2
    high, low = split(solved[:rows, :half] + solved[rows:, :half])
    rhs_part = solved[:rows, half:wide] + solved[:rows, wide + half :] + solved[rows:, half:wide]
    solution_buf[...] = rhs_part - dot(jnp.concatenate([high, high, low], axis=1), pivot)
    last = pltpu.make_async_copy(solution_buf, solution_out, sems.at[2 * PARTS * tiles])
    last.start()
    copies = []
    span = places // PARTS
    for tile in range(tiles):
        mine = sums[tile * kmax : (tile + 1) * kmax]
        high, low = split(mine[:, half:wide] + mine[:, wide + half :])
        gram = mine[:, :half].astype(BF16)
        weights = jnp.concatenate(
            [
                jnp.concatenate([gram, high], axis=1),
                jnp.concatenate([jnp.zeros_like(gram), low], axis=1),
            ],
            axis=0,
        )
        for part in range(PARTS):
            at = (tile, slice(None), pl.ds(part * span, span))
            product = dot_rows(weights, jnp.concatenate([left[at], left[at]], axis=0))
            left_buf[at] = product[:half].astype(BF16)
            rhs_buf[at] = side[at] - product[half:]
            for buf, hbm in ((left_buf, new_left), (rhs_buf, new_rhs)):
                copy = pltpu.make_async_copy(buf.at[at], hbm.at[at], sems.at[len(copies)])
                copy.start()
                copies.append(copy)

    for copy in copies + [last]:
        copy.wait()


def shards(
    count, panel_left, panel_right, ranks, rhs, pivot_left, pivot_right, finished, pivot_rhs, diag_inverse
):
    tiles, kmax, places = panel_left.shape
    rows, cols = pivot_right.shape
    nrhs = finished.shape[1]
    width = 2 * (cols + nrhs)
    params = pltpu.CompilerParams(vmem_limit_bytes=20 * 1024 * 1024)
    load_params = pltpu.CompilerParams(vmem_limit_bytes=56_000_000)
    block = pl.pallas_call(
        pack_kernel,
        out_shape=pltpu.VMEM((rows, width), F32),
        in_specs=[HBM] * 4,
        out_specs=VMEM,
        scratch_shapes=[
            pltpu.VMEM((rows, cols), BF16),
            pltpu.VMEM((rows, nrhs), F32),
            pltpu.VMEM((rows, cols), BF16),
            pltpu.VMEM((rows, nrhs), F32),
            pltpu.SemaphoreType.DMA((4,)),
        ],
        name="pack",
    )(pivot_right, finished, pivot_left, pivot_rhs)
    near, far = gather_halves(block, count)
    keep, inverse, left, side = pl.pallas_call(
        functools.partial(load_kernel, kmax),
        out_shape=(
            pltpu.VMEM((tiles * kmax, width), F32),
            pltpu.VMEM(diag_inverse.shape, F32),
            pltpu.VMEM(panel_left.shape, BF16),
            pltpu.VMEM(rhs.shape, F32),
        ),
        in_specs=[pl.BlockSpec(memory_space=pltpu.SMEM)] + [HBM] * 3,
        out_specs=(VMEM,) * 4,
        scratch_shapes=[pltpu.SemaphoreType.DMA((3,))],
        compiler_params=load_params,
        name="load",
    )(ranks, diag_inverse, panel_left, rhs)
    halves = [pltpu.VMEM((places // 2, width), BF16)] * 2
    middle = pl.pallas_call(
        functools.partial(first_kernel, [mask for _, mask in near]),
        out_shape=(
            pltpu.VMEM((tiles * kmax, width), F32),
            pltpu.VMEM((cols, width), F32),
            pltpu.VMEM((2 * rows, width), F32),
            pltpu.VMEM((2 * rows, places // 2), BF16),
        ),
        in_specs=[VMEM] * (len(near) + 2),
        out_specs=(VMEM,) * 4,
        scratch_shapes=halves,
        compiler_params=params,
        cost_estimate=pl.CostEstimate(flops=300_000_000, bytes_accessed=4_000_000, transcendentals=0),
        name="first",
    )(*[piece for piece, _ in near], panel_right, inverse)
    return pl.pallas_call(
        functools.partial(finish_kernel, [mask for _, mask in far]),
        out_shape=(
            jax.ShapeDtypeStruct(panel_left.shape, BF16),
            jax.ShapeDtypeStruct(rhs.shape, F32),
            jax.ShapeDtypeStruct((rows, nrhs), F32),
        ),
        in_specs=[VMEM] * (len(far) + 8),
        out_specs=(HBM,) * 3,
        scratch_shapes=halves
        + [
            pltpu.VMEM(panel_left.shape, BF16),
            pltpu.VMEM(rhs.shape, F32),
            pltpu.VMEM((rows, nrhs), F32),
            pltpu.SemaphoreType.DMA((2 * PARTS * tiles + 1,)),
        ],
        compiler_params=params,
        name="finish",
    )(*[piece for piece, _ in far], panel_right, keep, *middle, left, side)


def solution(mesh):
    count = mesh.shape[AXIS]
    tile = P(AXIS, None, None)
    row = P(AXIS, None)
    in_specs = (tile, tile, P(AXIS), tile, row, row, row, row, row)

    def local(*args):
        return shards(count, *args)

    step = jax.shard_map(local, mesh=mesh, in_specs=in_specs, out_specs=(tile, tile, row), check_vma=False)
    return step if squares(count) else step
```
